256 devices in a mesh: groups: 4 (over y, x), dp: 64 (over z, core).
Axes of the slice: x: 2, y: 2, z: 32, core: 2. Of those that a mesh axis runs over, the one named last changes fastest.
The devices are a block of a 4x8x32 slice.
Arguments:
- grads: bfloat16 [65536, 14336], P(('groups', 'dp')), parts along dimension 0, may hold values from -6 to 6
- inputs: bfloat16 [65536, 4096], P(('groups', 'dp')), parts along dimension 0, may hold values from -6 to 6
- lengths: int32 [512], P(('groups', 'dp')), parts along dimension 0, may hold values from 1 to 128
- left_rows: bfloat16 [3072, 14336], P(('groups', 'dp')), parts along dimension 0, may hold values from -0.046875 to 0.046875
- right_rows: bfloat16 [3072, 4096], P(('groups', 'dp')), parts along dimension 0, may hold values from -0.0014648438 to 0.0014648438
- owner_count: int32 [256], P(('groups', 'dp')), parts along dimension 0, may hold values from 0 to 12, as said below
Outputs:
- scores: float32 [512, 8], P(('groups', 'dp')), parts along dimension 0
The draws below stay inside these ranges and needn't reach their ends.
There are 4 independent parts, one for each index of `groups`. The reference program is written for one: setup_inputs(seed, part) draws one part's arguments, and reference() takes and returns one part's arrays. A program takes and returns all parts, laid end to end along the dimension named above; each array names one. Nothing has to cross between parts.
Inputs may be any that keep to these rules, and one draw needn't show every extreme that they name: Index i of dp holds live factor rows in its first owner_count[i] slots, the rows offset_i to offset_i + owner_count[i] - 1 where offset_i is the sum of the counts of lower indices. The counts sum to 256, and some index holds 12.
All inputs are finite; a program needn't handle non-finite values.
Results may differ from the reference program's by a relative error of at most 0.0003.
Values may be sent and summed in bfloat16 or wider, within the bound.
No kernel may reach another device: no remote copies, remote signals or barrier semaphores. Data moves between devices by JAX's collectives and lax.ppermute only.
A program may use at most 192 MiB of HBM per device.

```python
import jax
import jax.numpy as jnp
from jax import lax

D = 4096
FF = 14336
RANK = 32
LEN = 128
ROWS_DEV = 4
CAP = 12
SLOTS = 768
EXAMPLES = 128
TOKENS = 16384
N_DP = 64


def draw_owner_count(key, part):
    total_rows = ROWS_DEV * N_DP
    slot_total = CAP * N_DP
    key_first, key_order = jax.random.split(jax.random.fold_in(key, 7))
    forced = jax.random.randint(key_first, (), 0, N_DP)
    priority = jax.random.permutation(key_order, slot_total).astype(jnp.int32)
    owner_ids = jnp.arange(slot_total, dtype=jnp.int32) // CAP
    priority = jnp.where(owner_ids == forced, priority - slot_total, priority)
    ranked = jnp.argsort(jnp.argsort(priority))
    chosen = (ranked < total_rows).astype(jnp.int32)
    return jnp.sum(chosen.reshape(N_DP, CAP), axis=1).astype(jnp.int32)


def touch_ends(values, own_key, least, largest):
    extent = values.shape
    index_at = [jax.random.randint(jax.random.fold_in(own_key, axis), (), 0, extent[axis]) for axis in range(len(extent))]
    values = values.at[tuple(index_at)].set(least)
    longest = extent.index(max(extent))
    index_at[longest] = (index_at[longest] + 1) % extent[longest]
    return values.at[tuple(index_at)].set(largest)


def shard_levels(rng, dims, cuts, low, top_value):
    def one(position, blocks):
        draws = jax.random.uniform(jax.random.fold_in(jax.random.fold_in(rng, 6), position), (blocks,), jnp.float32, low / len(cuts), top_value / len(cuts))
        return jnp.repeat(jnp.exp(draws), dims[position] // blocks).reshape((-1,) + (1,) * (len(dims) - position - 1))

    factor_of = one(*cuts[0])
    for cut in cuts[1:]:
        factor_of = factor_of * one(*cut)
    return factor_of


def bell_draw(own_key, dims, deviation, limit, shards=(), held_as=jnp.bfloat16):
    entries = jax.random.normal(own_key, dims, jnp.float32) * deviation
    if len(shards) > 0:
        entries = shard_levels(own_key, dims, shards, -0.22, 0.18) * entries
    return jnp.clip(entries, min=-limit, max=limit).astype(held_as)


def setup_inputs(seed: int = 0, part: int = 0) -> dict:
    key_list = jax.random.split(jax.random.key(seed), 7)
    own_keys = jax.random.split(jax.random.fold_in(key_list[6], part), 7)
    return {
        "grads": bell_draw(own_keys[0], (TOKENS, FF), 1.0, 6.0, ((0, 64),)),
        "inputs": bell_draw(own_keys[1], (TOKENS, D), 1.0, 6.0, ((0, 64),)),
        "lengths": touch_ends(jax.random.randint(own_keys[2], (EXAMPLES,), 1, LEN + 1), jax.random.fold_in(own_keys[2], 1), 1, LEN).astype(jnp.int32),
        "left_rows": bell_draw(own_keys[3], (SLOTS, FF), FF ** -0.5, 0.046875, ((0, 64),)),
        "right_rows": bell_draw(own_keys[4], (SLOTS, D), (D * RANK * LEN) ** -0.5, 0.0014648438, ((0, 64),)),
        "owner_count": draw_owner_count(jax.random.fold_in(jax.random.fold_in(key_list[6], part), 71), part),
    }


def reference(grads, inputs, lengths, left_rows, right_rows, owner_count):
    devices = owner_count.shape[0]
    capacity = left_rows.shape[0] // devices
    queries = devices * ROWS_DEV // RANK
    offsets = jnp.cumsum(owner_count) - owner_count
    slot_ids = jnp.arange(devices * capacity, dtype=jnp.int32)
    within = slot_ids % capacity
    owner_ids = slot_ids // capacity
    held_rows = owner_count[owner_ids]
    first_row = offsets[owner_ids]
    query_ids = (first_row + within) // RANK
    assign = ((query_ids[:, None] == jnp.arange(queries, dtype=jnp.int32)[None, :]) & (within < held_rows)[:, None]).astype(jnp.float32)
    live_tokens = (jnp.arange(LEN, dtype=jnp.int32)[None, :] < lengths[:, None]).astype(jnp.float32).reshape(-1)
    left_proj = jnp.dot(grads, left_rows.T, preferred_element_type=jnp.float32)
    right_proj = jnp.dot(inputs, right_rows.T, preferred_element_type=jnp.float32)
    joined = left_proj * right_proj * live_tokens[:, None]
    example_sums = jnp.sum(joined.reshape(-1, LEN, joined.shape[1]), axis=1)
    return jnp.dot(example_sums, assign, precision=lax.Precision.HIGHEST)
```

```python
import jax
import jax.numpy as jnp
from jax import lax
from jax.sharding import Mesh
from jax.sharding import PartitionSpec as P

RANK = 32
LEN = 128
ROWS_DEV = 4
REACH = 2
CHAINS = 2
PART = ("z", "core")
SPLIT = ("groups", "z", "core")
CONTRACT = (((1,), (1,)), ((), ()))
FLAT = (((1,), (0,)), ((), ()))


def two_way(chips, hops):
    right = [(2 * i + 1, 2 * ((i + hops) % chips) + 1) for i in range(chips)]
    left = [(2 * i, 2 * ((i - hops) % chips)) for i in range(chips)]
    return right + left


def swap(x):
    return lax.ppermute(x, "core", [(0, 1), (1, 0)])


def dot(a, b):
    return lax.dot_general(a, b, CONTRACT, preferred_element_type=jnp.float32)


def sums_of(grads, inputs, live, left, right):
    joined = dot(grads, left) * dot(inputs, right) * live[:, None]
    return jnp.sum(joined.reshape(-1, LEN, joined.shape[1]), axis=1)


def exact(sums, assign):
    return jnp.dot(sums, assign, precision=lax.Precision.HIGHEST)


def on_device(grads, inputs, lengths, left_rows, right_rows, owner_count):
    chips = lax.axis_size("z")
    z = lax.axis_index("z")
    core = lax.axis_index("core")
    devices = 2 * chips
    total = devices * ROWS_DEV
    queries = total // RANK
    block = total // chips
    cap = left_rows.shape[0]
    ff = left_rows.shape[1]
    width = ff + right_rows.shape[1]
    half = width // 2
    live = (jnp.arange(LEN, dtype=jnp.int32)[None, :] < lengths[:, None]).astype(jnp.float32).reshape(-1)

    own = jnp.concatenate([left_rows, right_rows], axis=1)
    packed = jnp.concatenate([own[:, :half], own[:, half:]], axis=0)
    other = swap(packed)
    other = jnp.concatenate([other[:cap], other[cap:]], axis=1)
    first = core == 0
    raw = jnp.concatenate([jnp.where(first, own, other), jnp.where(first, other, own)], axis=0)

    own_count = owner_count[0].astype(jnp.float32)
    other_count = swap(jnp.broadcast_to(own_count, (8, 128)))[0, 0]
    n0 = jnp.where(first, own_count, other_count).astype(jnp.int32)
    n1 = jnp.where(first, other_count, own_count).astype(jnp.int32)
    slot = jnp.arange(2 * cap, dtype=jnp.int32)
    second = slot >= cap
    within = jnp.where(second, slot - cap, slot)
    valid = within < jnp.where(second, n1, n0)
    rank = jnp.where(valid, within + jnp.where(second, n0, 0), -1)
    lead = jnp.where(first, 0, n0 + n1 - 2 * block)
    edge_at = jnp.arange(2 * block, dtype=jnp.int32) + lead
    pick = (valid[None, :] & (rank[None, :] == edge_at[:, None])).astype(jnp.bfloat16)
    edge = lax.dot_general(pick, raw, FLAT, preferred_element_type=jnp.float32).astype(jnp.bfloat16)
    tip = jnp.where(first, edge[:block], edge[block:])
    me = 2 * z + core
    device_list = jnp.arange(devices, dtype=jnp.int32)
    one_hop = lax.ppermute(edge, PART, two_way(chips, 1))
    two_hops = lax.ppermute(tip, PART, two_way(chips, 2))
    counts = lax.psum(jnp.where(device_list == me, owner_count[0], 0), PART)
    one_hop, two_hops, counts = lax.optimization_barrier((one_hop, two_hops, counts))
    counts, grads_t, inputs_t, live_t = lax.optimization_barrier((counts, grads, inputs, live))
    grads_s, inputs_s, live_s = swap(grads_t), swap(inputs_t), swap(live_t)
    pair = counts.reshape(chips, 2)
    held = jnp.sum(pair, axis=1)
    chip_list = jnp.arange(chips, dtype=jnp.int32)
    before = jnp.sum(jnp.where(chip_list[None, :] < chip_list[:, None], held[None, :], 0), axis=1)
    drift = before - block * chip_list
    low = jnp.min(drift)
    high = jnp.max(drift + held - 1)
    span = block * (2 * REACH + 1) - 1
    shift = jnp.floor_divide(block - 1 - low - high, 2)
    fits = high - low <= span

    place = jnp.arange(block, dtype=jnp.int32)
    side = jnp.where(first, 1, -1)

    def at(values, chip):
        return jnp.sum(jnp.where(chip_list == chip, values, 0))

    def chosen(rows, ranks, good, hops):
        source = jnp.remainder(z + side * hops, chips)
        spot = at(drift, source) + shift + block * side * hops + ranks
        sel = (good & (spot[None, :] == place[:, None])).astype(jnp.bfloat16)
        return lax.dot_general(sel, rows, FLAT, preferred_element_type=jnp.float32)

    def arrived(rows, hops):
        held_there = at(held, jnp.remainder(z + side * hops, chips))
        size = rows.shape[0]
        ranks = jnp.arange(size, dtype=jnp.int32) + jnp.where(first, 0, held_there - size)
        return chosen(rows, ranks, ((ranks >= 0) & (ranks < held_there))[None, :], hops)

    mine = chosen(raw, rank, (valid & ~first)[None, :], 0) + arrived(one_hop, 1) + arrived(two_hops, 2)
    mine = mine.astype(jnp.bfloat16)
    mine = mine + swap(mine)

    steps = chips // 2
    piece = width // CHAINS
    chains = [[mine[:, i * piece : (i + 1) * piece]] for i in range(CHAINS)]
    for k in range(steps):
        for i, chain in enumerate(chains):
            before_it = chains[i - 1]
            j = k if i > 0 else k - 1
            if j > 0:
                chain[k], before_it[j] = lax.optimization_barrier((chain[k], before_it[j]))
            chain.append(lax.ppermute(chain[k], PART, two_way(chips, 1)))
    stacked = []
    for chain in chains:
        head = jnp.where(first, chain[0], chain[-1])
        stacked.append(jnp.concatenate([head] + chain[1:-1], axis=0))
    rows = jnp.concatenate(stacked, axis=1)
    left, right = rows[:, :ff], rows[:, ff:]

    hop = jnp.repeat(jnp.arange(steps, dtype=jnp.int32), block)
    hop = jnp.where(first, hop, -jnp.where(hop == 0, steps, hop))
    position = block * (z + hop) + jnp.tile(place, steps)
    query = jnp.remainder(position - shift, total) // RANK
    assign = (query[:, None] == jnp.arange(queries, dtype=jnp.int32)[None, :]).astype(jnp.float32)
    ours = exact(sums_of(grads, inputs, live, left, right), assign)
    theirs = exact(sums_of(grads_s, inputs_s, live_s, left, right), assign)
    fast = ours + swap(theirs)

    def general(fast, grads, inputs, live, raw):
        def step(k, carry):
            rows, out = carry
            source = jnp.remainder(z - k, chips)
            here = chip_list == source
            c0 = jnp.sum(jnp.where(here, pair[:, 0], 0))
            c1 = jnp.sum(jnp.where(here, pair[:, 1], 0))
            begin = jnp.sum(jnp.where(here, before, 0))
            valid = within < jnp.where(second, c1, c0)
            owner = (begin + within + jnp.where(second, c0, 0)) // RANK
            match = (owner[:, None] == jnp.arange(queries, dtype=jnp.int32)[None, :]) & valid[:, None]
            sums = sums_of(grads, inputs, live, rows[:, :ff], rows[:, ff:])
            out = out + exact(sums, match.astype(jnp.float32))
            return lax.ppermute(rows, "z", [(i, (i + 1) % chips) for i in range(chips)]), out

        return lax.fori_loop(0, chips, step, (raw, jnp.zeros_like(fast)))[1]

    return lax.cond(fits, lambda f, *_: f, general, fast, grads, inputs, live, raw)


def solution(mesh):
    groups, dp = mesh.devices.shape
    finer = Mesh(mesh.devices.reshape(groups, dp // 2, 2), SPLIT)
    return jax.shard_map(
        on_device,
        mesh=finer,
        in_specs=(
            P(SPLIT, None),
            P(SPLIT, None),
            P(SPLIT),
            P(SPLIT, None),
            P(SPLIT, None),
            P(SPLIT),
        ),
        out_specs=P(SPLIT, None),
        check_vma=False,
    )
```

```python
import jax
import jax.numpy as jnp
from jax import lax
from jax.experimental import pallas as pl
from jax.experimental.pallas import tpu as pltpu
from jax.sharding import Mesh
from jax.sharding import PartitionSpec as P

RANK = 32
LEN = 128
LANES = 128
ROWS_DEV = 4
REACH = 2
CHAINS = 2
STRIP = 1024
PART = ("z", "core")
SPLIT = ("groups", "z", "core")
CONTRACT = (((1,), (1,)), ((), ()))
FLAT = (((1,), (0,)), ((), ()))


def two_way(chips, hops):
    right = [(2 * i + 1, 2 * ((i + hops) % chips) + 1) for i in range(chips)]
    left = [(2 * i, 2 * ((i - hops) % chips)) for i in range(chips)]
    return right + left


def swap(x):
    return lax.ppermute(x, "core", [(0, 1), (1, 0)])


def dot(a, b):
    return lax.dot_general(a, b, CONTRACT, preferred_element_type=jnp.float32)


def sums_of(grads, inputs, live, left, right):
    joined = dot(grads, left) * dot(inputs, right) * live[:, None]
    return jnp.sum(joined.reshape(-1, LEN, joined.shape[1]), axis=1)


def exact(sums, assign):
    return jnp.dot(sums, assign, precision=lax.Precision.HIGHEST)


def scored(blocks, grads, inputs, lens, assign):
    block = blocks[0][0].shape[0]
    flat = [(s, p, len(pieces), x) for s, pieces in enumerate(blocks) for p, x in enumerate(pieces)]
    tokens, ff = grads[0].shape
    width = ff + inputs[0].shape[1]
    rows, queries = assign.shape
    sides = len(grads)
    examples = sides * tokens // LEN
    wide = ff // STRIP
    steps = width // STRIP

    def body(lens_ref, *refs):
        (g0, g1, i0, i1, assign_ref), refs = refs[:5], refs[5:]
        parts, refs = refs[: len(flat)], refs[len(flat) :]
        out_ref, held, left, right, sems = refs
        k = pl.program_id(0)

        def move(i):
            s, p, n, x = flat[i]
            target = held.at[pl.ds(s * block, block), pl.ds(p * (width // n), width // n)]
            return pltpu.make_async_copy(parts[i], target, sems.at[i])

        @pl.when(k == 0)
        def _():
            for i in range(len(flat)):
                move(i).start()
            left[...] = jnp.zeros_like(left)
            right[...] = jnp.zeros_like(right)

            for i, (_, p, _, _) in enumerate(flat):
                if p == 0:
                    move(i).wait()

        @pl.when(k == width // CHAINS // STRIP)
        def _():
            for i, (_, p, _, _) in enumerate(flat):
                if p > 0:
                    move(i).wait()

        strip = held[:, pl.ds(k * STRIP, STRIP)]

        @pl.when(k < wide)
        def _():
            left[:tokens, :] += dot(g0[...], strip)
            left[tokens:, :] += dot(g1[...], strip)

        @pl.when(k >= wide)
        def _():
            right[:tokens, :] += dot(i0[...], strip)
            right[tokens:, :] += dot(i1[...], strip)

        @pl.when(k == steps - 1)
        def _():
            token = lax.broadcasted_iota(jnp.int32, (LEN, rows), 0)
            sums = []
            for e in range(examples):
                at = pl.ds(e * LEN, LEN)
                joined = left[at, :] * right[at, :]
                sums.append(jnp.sum(jnp.where(token < lens_ref[e], joined, 0.0), axis=0, keepdims=True))
            sums = jnp.concatenate(sums + [jnp.zeros_like(sums[0])] * (8 - examples), axis=0)
            out_ref[...] = exact(sums, assign_ref[...])

    wide_spec = pl.BlockSpec((tokens, STRIP), lambda k, _: (0, jnp.minimum(k, wide - 1)))
    slim_spec = pl.BlockSpec((tokens, STRIP), lambda k, _: (0, jnp.maximum(k - wide, 0)))
    whole = pl.BlockSpec((rows, queries), lambda k, _: (0, 0))
    anywhere = pl.BlockSpec(memory_space=pl.ANY)
    return pl.pallas_call(
        body,
        out_shape=jax.ShapeDtypeStruct((8, queries), jnp.float32),
        grid_spec=pltpu.PrefetchScalarGridSpec(
            num_scalar_prefetch=1,
            grid=(steps,),
            in_specs=[wide_spec, wide_spec, slim_spec, slim_spec, whole] + [anywhere] * len(flat),
            out_specs=pl.BlockSpec((8, queries), lambda k, _: (0, 0)),
            scratch_shapes=[
                pltpu.VMEM((rows, width), jnp.bfloat16),
                pltpu.VMEM((sides * tokens, rows), jnp.float32),
                pltpu.VMEM((sides * tokens, rows), jnp.float32),
                pltpu.SemaphoreType.DMA((len(flat),)),
            ],
        ),
        compiler_params=pltpu.CompilerParams(dimension_semantics=("arbitrary",)),
    )(lens, *grads, *inputs, assign, *[x for *_, x in flat])


def on_device(grads, inputs, lengths, left_rows, right_rows, owner_count):
    chips = lax.axis_size("z")
    z = lax.axis_index("z")
    core = lax.axis_index("core")
    devices = 2 * chips
    total = devices * ROWS_DEV
    queries = total // RANK
    block = total // chips
    cap = left_rows.shape[0]
    ff = left_rows.shape[1]
    width = ff + right_rows.shape[1]
    half = width // 2
    live = (jnp.arange(LEN, dtype=jnp.int32)[None, :] < lengths[:, None]).astype(jnp.float32).reshape(-1)

    own = jnp.concatenate([left_rows, right_rows], axis=1)
    packed = jnp.concatenate([own[:, :half], own[:, half:]], axis=0)
    small = jnp.concatenate([owner_count, lengths, jnp.zeros((LANES - 1 - lengths.shape[0],), jnp.int32)])
    notes = jnp.broadcast_to(small.astype(jnp.bfloat16)[None, :], (2 * cap, LANES))
    other = swap(jnp.concatenate([packed, notes], axis=1))
    notes = other[0, half:].astype(jnp.int32)
    other_count, lengths_s = notes[0], notes[1 : 1 + lengths.shape[0]]
    other = jnp.concatenate([other[:cap, :half], other[cap:, :half]], axis=1)
    first = core == 0
    raw = jnp.concatenate([jnp.where(first, own, other), jnp.where(first, other, own)], axis=0)

    n0 = jnp.where(first, owner_count[0], other_count)
    n1 = jnp.where(first, other_count, owner_count[0])
    slot = jnp.arange(2 * cap, dtype=jnp.int32)
    second = slot >= cap
    within = jnp.where(second, slot - cap, slot)
    valid = within < jnp.where(second, n1, n0)
    rank = jnp.where(valid, within + jnp.where(second, n0, 0), -1)
    lead = jnp.where(first, 0, n0 + n1 - 2 * block)
    edge_at = jnp.arange(2 * block, dtype=jnp.int32) + lead
    pick = (valid[None, :] & (rank[None, :] == edge_at[:, None])).astype(jnp.bfloat16)
    edge = lax.dot_general(pick, raw, FLAT, preferred_element_type=jnp.float32).astype(jnp.bfloat16)
    tip = jnp.where(first, edge[:block], edge[block:])
    me = 2 * z + core
    device_list = jnp.arange(devices, dtype=jnp.int32)
    one_hop = lax.ppermute(edge, PART, two_way(chips, 1))
    two_hops = lax.ppermute(tip, PART, two_way(chips, 2))
    counts = lax.psum(jnp.where(device_list == me, owner_count[0], 0), PART)
    one_hop, two_hops, counts = lax.optimization_barrier((one_hop, two_hops, counts))
    counts, grads_t, inputs_t = lax.optimization_barrier((counts, grads, inputs))
    grads_s, inputs_s = swap(grads_t), swap(inputs_t)
    pair = counts.reshape(chips, 2)
    held = jnp.sum(pair, axis=1)
    chip_list = jnp.arange(chips, dtype=jnp.int32)
    before = jnp.sum(jnp.where(chip_list[None, :] < chip_list[:, None], held[None, :], 0), axis=1)
    drift = before - block * chip_list
    low = jnp.min(drift)
    high = jnp.max(drift + held - 1)
    span = block * (2 * REACH + 1) - 1
    shift = jnp.floor_divide(block - 1 - low - high, 2)
    fits = high - low <= span

    place = jnp.arange(block, dtype=jnp.int32)
    side = jnp.where(first, 1, -1)

    def at(values, chip):
        return jnp.sum(jnp.where(chip_list == chip, values, 0))

    def chosen(rows, ranks, good, hops):
        source = jnp.remainder(z + side * hops, chips)
        spot = at(drift, source) + shift + block * side * hops + ranks
        sel = (good & (spot[None, :] == place[:, None])).astype(jnp.bfloat16)
        return lax.dot_general(sel, rows, FLAT, preferred_element_type=jnp.float32)

    def arrived(rows, hops):
        held_there = at(held, jnp.remainder(z + side * hops, chips))
        size = rows.shape[0]
        ranks = jnp.arange(size, dtype=jnp.int32) + jnp.where(first, 0, held_there - size)
        return chosen(rows, ranks, ((ranks >= 0) & (ranks < held_there))[None, :], hops)

    mine = chosen(raw, rank, (valid & ~first)[None, :], 0) + arrived(one_hop, 1) + arrived(two_hops, 2)
    mine = mine.astype(jnp.bfloat16)
    mine = mine + swap(mine)

    steps = chips // 2
    piece = width // CHAINS
    forth = two_way(chips, 1)
    near = lax.ppermute(mine, PART, forth)
    chains = [[near[:, i * piece : (i + 1) * piece]] for i in range(CHAINS)]
    for k in range(steps - 2):
        for i, chain in enumerate(chains):
            before_it = chains[i - 1]
            j = k if i > 0 else k - 1
            if j > 0:
                chain[k], before_it[j] = lax.optimization_barrier((chain[k], before_it[j]))
            chain.append(lax.ppermute(chain[k], PART, forth))
    last = lax.ppermute(jnp.concatenate([c[-1] for c in chains], axis=1), PART, forth)
    blocks = [[mine], [near]] + [[c[j] for c in chains] for j in range(1, steps - 1)] + [[last]]

    hop = jnp.repeat(jnp.arange(steps + 1, dtype=jnp.int32), block)
    counted = jnp.where(first, hop < steps, hop > 0)
    position = block * (z + jnp.where(first, hop, -hop)) + jnp.tile(place, steps + 1)
    query = jnp.remainder(position - shift, total) // RANK
    assign = (query[:, None] == jnp.arange(queries, dtype=jnp.int32)[None, :]) & counted[:, None]
    lens = jnp.concatenate([lengths, lengths_s])
    both = scored(blocks, (grads, grads_s), (inputs, inputs_s), lens, assign.astype(jnp.float32))
    mine_n = lengths.shape[0]
    fast = both[:mine_n] + swap(both[mine_n : 2 * mine_n])

    def general(fast, grads, inputs, live, raw):
        def step(k, carry):
            rows, out = carry
            source = jnp.remainder(z - k, chips)
            here = chip_list == source
            c0 = jnp.sum(jnp.where(here, pair[:, 0], 0))
            c1 = jnp.sum(jnp.where(here, pair[:, 1], 0))
            begin = jnp.sum(jnp.where(here, before, 0))
            valid = within < jnp.where(second, c1, c0)
            owner = (begin + within + jnp.where(second, c0, 0)) // RANK
            match = (owner[:, None] == jnp.arange(queries, dtype=jnp.int32)[None, :]) & valid[:, None]
            sums = sums_of(grads, inputs, live, rows[:, :ff], rows[:, ff:])
            out = out + exact(sums, match.astype(jnp.float32))
            return lax.ppermute(rows, "z", [(i, (i + 1) % chips) for i in range(chips)]), out

        return lax.fori_loop(0, chips, step, (raw, jnp.zeros_like(fast)))[1]

    return lax.cond(fits, lambda f, *_: f, general, fast, grads, inputs, live, raw)


def solution(mesh):
    groups, dp = mesh.devices.shape
    finer = Mesh(mesh.devices.reshape(groups, dp // 2, 2), SPLIT)
    return jax.shard_map(
        on_device,
        mesh=finer,
        in_specs=(
            P(SPLIT, None),
            P(SPLIT, None),
            P(SPLIT),
            P(SPLIT, None),
            P(SPLIT, None),
            P(SPLIT),
        ),
        out_specs=P(SPLIT, None),
        check_vma=False,
    )
```

```python
import jax
import jax.numpy as jnp
from jax import lax
from jax.experimental import pallas as pl
from jax.experimental.pallas import tpu as pltpu
from jax.sharding import Mesh
from jax.sharding import PartitionSpec as P

RANK = 32
LEN = 128
LANES = 128
ROWS_DEV = 4
REACH = 2
CHAINS = 2
PARTS = 3
STRIP = 2048
PART = ("z", "core")
SPLIT = ("groups", "z", "core")
CONTRACT = (((1,), (1,)), ((), ()))
FLAT = (((1,), (0,)), ((), ()))


def two_way(chips, hops):
    right = [(2 * i + 1, 2 * ((i + hops) % chips) + 1) for i in range(chips)]
    left = [(2 * i, 2 * ((i - hops) % chips)) for i in range(chips)]
    return right + left


def swap(x):
    return lax.ppermute(x, "core", [(0, 1), (1, 0)])


def dot(a, b):
    return lax.dot_general(a, b, CONTRACT, preferred_element_type=jnp.float32)


def sums_of(grads, inputs, live, left, right):
    joined = dot(grads, left) * dot(inputs, right) * live[:, None]
    return jnp.sum(joined.reshape(-1, LEN, joined.shape[1]), axis=1)


def exact(sums, assign):
    return jnp.dot(sums, assign, precision=lax.Precision.HIGHEST)


def log2(n):
    assert n & (n - 1) == 0
    return n.bit_length() - 1


def routed_rows(raw, one_hop, two_hops, counts, seat, block):
    chips = counts.shape[0] // 2
    slots, width = raw.shape
    cap = slots // 2
    strip = width // PARTS

    def body(counts_ref, seat_ref, raw_ref, one_ref, two_ref, out_ref, routed_ref, sel_ref, drift):
        @pl.when(pl.program_id(0) == 0)
        def _():
            z, first = seat_ref[0], seat_ref[1] == 0
            before, low, high = jnp.int32(0), jnp.int32(0), jnp.int32(0)
            for y in range(chips):
                drift[y] = before - block * y
                low = jnp.minimum(low, drift[y])
                before += counts_ref[2 * y] + counts_ref[2 * y + 1]
                high = jnp.maximum(high, before - 1 - block * y)
            shift = (block - 1 - low - high) >> 1
            routed_ref[0] = shift
            routed_ref[1] = (high - low <= block * (2 * REACH + 1) - 1).astype(jnp.int32)
            side = jnp.where(first, 1, -1)
            for h, size in enumerate((slots, 2 * block, block)):
                source = (z + side * h) & (chips - 1)
                c0, c1 = counts_ref[2 * source], counts_ref[2 * source + 1]
                start = drift[source] + shift + block * side * h
                slot = lax.broadcasted_iota(jnp.int32, (block, size), 1)
                place = lax.broadcasted_iota(jnp.int32, (block, size), 0)
                if h == 0:
                    second = slot >= cap
                    within = jnp.where(second, slot - cap, slot)
                    rank = within + jnp.where(second, c0, 0)
                    good = (within < jnp.where(second, c1, c0)) & (rank + jnp.where(first, 2 * slots, 0) < 2 * slots)
                else:
                    rank = slot + jnp.where(first, 0, c0 + c1 - size)
                    good = (rank >= 0) & (rank < c0 + c1)
                sel_ref[h, :, :size] = (good & (start + rank == place)).astype(jnp.float32)

        taken = None
        for h, ref in enumerate((raw_ref, one_ref, two_ref)):
            sel = sel_ref[h, :, : ref.shape[0]].astype(jnp.bfloat16)
            part = lax.dot_general(sel, ref[...], FLAT, preferred_element_type=jnp.float32)
            taken = part if taken is None else taken + part
        out_ref[...] = taken.astype(jnp.bfloat16)

    log2(chips)

    def spec(size):
        return pl.BlockSpec((size, strip), lambda k, *_: (0, k))

    return pl.pallas_call(
        body,
        out_shape=(jax.ShapeDtypeStruct((block, width), jnp.bfloat16), jax.ShapeDtypeStruct((2,), jnp.int32)),
        grid_spec=pltpu.PrefetchScalarGridSpec(
            num_scalar_prefetch=2,
            grid=(PARTS,),
            in_specs=[spec(slots), spec(2 * block), spec(block)],
            out_specs=(spec(block), pl.BlockSpec(memory_space=pltpu.SMEM)),
            scratch_shapes=[pltpu.VMEM((3, block, LANES), jnp.float32), pltpu.SMEM((chips,), jnp.int32)],
        ),
        compiler_params=pltpu.CompilerParams(dimension_semantics=("arbitrary",)),
    )(counts, seat, raw, one_hop, two_hops)


def scored(blocks, grads, inputs, lens, seat, routed, chips, total):
    block = blocks[0][0].shape[0]
    flat = [(s, p, len(pieces), x) for s, pieces in enumerate(blocks) for p, x in enumerate(pieces)]
    tokens, ff = grads[0].shape
    width = ff + inputs[0].shape[1]
    rows = len(blocks) * block
    queries = total // RANK
    sides = len(grads)
    examples = sides * tokens // LEN
    wide = ff // STRIP
    steps = width // STRIP

    def body(lens_ref, seat_ref, routed_ref, *refs):
        (g0, g1, i0, i1), refs = refs[:4], refs[4:]
        parts, refs = refs[: len(flat)], refs[len(flat) :]
        out_ref, held, left, right, sems = refs
        k = pl.program_id(0)

        def move(i):
            s, p, n, x = flat[i]
            target = held.at[pl.ds(s * block, block), pl.ds(p * (width // n), width // n)]
            return pltpu.make_async_copy(parts[i], target, sems.at[i])

        @pl.when(k == 0)
        def _():
            for i in range(len(flat)):
                move(i).start()
            left[...] = jnp.zeros_like(left)
            right[...] = jnp.zeros_like(right)

            for i, (_, p, _, _) in enumerate(flat):
                if p == 0:
                    move(i).wait()

        @pl.when(k == width // CHAINS // STRIP)
        def _():
            for i, (_, p, _, _) in enumerate(flat):
                if p > 0:
                    move(i).wait()

        strip = held[:, pl.ds(k * STRIP, STRIP)]

        @pl.when(k < wide)
        def _():
            left[:tokens, :] += dot(g0[...], strip)
            left[tokens:, :] += dot(g1[...], strip)

        @pl.when(k >= wide)
        def _():
            right[:tokens, :] += dot(i0[...], strip)
            right[tokens:, :] += dot(i1[...], strip)

        @pl.when(k == steps - 1)
        def _():
            token = lax.broadcasted_iota(jnp.int32, (LEN, rows), 0)
            sums = []
            for e in range(examples):
                at = pl.ds(e * LEN, LEN)
                joined = left[at, :] * right[at, :]
                sums.append(jnp.sum(jnp.where(token < lens_ref[e], joined, 0.0), axis=0, keepdims=True))
            sums = jnp.concatenate(sums + [jnp.zeros_like(sums[0])] * (8 - examples), axis=0)
            row = lax.broadcasted_iota(jnp.int32, (rows, queries), 0)
            hop = row >> log2(block)
            first = seat_ref[1] == 0
            chip = seat_ref[0] + jnp.where(first, hop, -hop)
            position = block * chip + (row & (block - 1)) - routed_ref[0]
            query = (position & (total - 1)) >> log2(RANK)
            counted = (hop >= jnp.where(first, 0, 1)) & (hop < jnp.where(first, chips // 2, chips))
            match = (query == lax.broadcasted_iota(jnp.int32, (rows, queries), 1)) & counted
            out_ref[...] = exact(sums, match.astype(jnp.float32))

    wide_spec = pl.BlockSpec((tokens, STRIP), lambda k, *_: (0, jnp.minimum(k, wide - 1)))
    slim_spec = pl.BlockSpec((tokens, STRIP), lambda k, *_: (0, jnp.maximum(k - wide, 0)))
    anywhere = pl.BlockSpec(memory_space=pl.ANY)
    return pl.pallas_call(
        body,
        out_shape=jax.ShapeDtypeStruct((8, queries), jnp.float32),
        grid_spec=pltpu.PrefetchScalarGridSpec(
            num_scalar_prefetch=3,
            grid=(steps,),
            in_specs=[wide_spec, wide_spec, slim_spec, slim_spec] + [anywhere] * len(flat),
            out_specs=pl.BlockSpec((8, queries), lambda k, *_: (0, 0)),
            scratch_shapes=[
                pltpu.VMEM((rows, width), jnp.bfloat16),
                pltpu.VMEM((sides * tokens, rows), jnp.float32),
                pltpu.VMEM((sides * tokens, rows), jnp.float32),
                pltpu.SemaphoreType.DMA((len(flat),)),
            ],
        ),
        compiler_params=pltpu.CompilerParams(dimension_semantics=("arbitrary",)),
    )(lens, seat, routed, *grads, *inputs, *[x for *_, x in flat])


def on_device(grads, inputs, lengths, left_rows, right_rows, owner_count):
    chips = lax.axis_size("z")
    z = lax.axis_index("z")
    core = lax.axis_index("core")
    devices = 2 * chips
    total = devices * ROWS_DEV
    queries = total // RANK
    block = total // chips
    cap = left_rows.shape[0]
    ff = left_rows.shape[1]
    width = ff + right_rows.shape[1]
    half = width // 2
    live = (jnp.arange(LEN, dtype=jnp.int32)[None, :] < lengths[:, None]).astype(jnp.float32).reshape(-1)

    own = jnp.concatenate([left_rows, right_rows], axis=1)
    packed = jnp.concatenate([own[:, :half], own[:, half:]], axis=0)
    small = jnp.concatenate([owner_count, lengths, jnp.zeros((LANES - 1 - lengths.shape[0],), jnp.int32)])
    notes = jnp.broadcast_to(small.astype(jnp.bfloat16)[None, :], (2 * cap, LANES))
    other = swap(jnp.concatenate([packed, notes], axis=1))
    notes = other[0, half:].astype(jnp.int32)
    other_count, lengths_s = notes[0], notes[1 : 1 + lengths.shape[0]]
    other = jnp.concatenate([other[:cap, :half], other[cap:, :half]], axis=1)
    first = core == 0
    raw = jnp.concatenate([jnp.where(first, own, other), jnp.where(first, other, own)], axis=0)

    n0 = jnp.where(first, owner_count[0], other_count)
    n1 = jnp.where(first, other_count, owner_count[0])
    slot = jnp.arange(2 * cap, dtype=jnp.int32)
    second = slot >= cap
    within = jnp.where(second, slot - cap, slot)
    valid = within < jnp.where(second, n1, n0)
    rank = jnp.where(valid, within + jnp.where(second, n0, 0), -1)
    lead = jnp.where(first, 0, n0 + n1 - 2 * block)
    edge_at = jnp.arange(2 * block, dtype=jnp.int32) + lead
    pick = (valid[None, :] & (rank[None, :] == edge_at[:, None])).astype(jnp.bfloat16)
    edge = lax.dot_general(pick, raw, FLAT, preferred_element_type=jnp.float32).astype(jnp.bfloat16)
    tip = jnp.where(first, edge[:block], edge[block:])
    device_list = jnp.arange(devices, dtype=jnp.int32)
    one_hop = lax.ppermute(edge, PART, two_way(chips, 1))
    two_hops = lax.ppermute(tip, PART, two_way(chips, 2))
    held_here = jnp.where(device_list == 2 * z, n0, jnp.where(device_list == 2 * z + 1, n1, 0))
    counts = lax.psum(held_here, "z")
    one_hop, two_hops, counts = lax.optimization_barrier((one_hop, two_hops, counts))
    counts, grads_t, inputs_t = lax.optimization_barrier((counts, grads, inputs))
    grads_s, inputs_s = swap(grads_t), swap(inputs_t)
    seat = jnp.stack([z, core]).astype(jnp.int32)
    mine, routed = routed_rows(raw, one_hop, two_hops, counts, seat, block)
    mine = mine + swap(mine)

    steps = chips // 2
    piece = width // CHAINS
    forth = two_way(chips, 1)
    near = lax.ppermute(mine, PART, forth)
    chains = [[near[:, i * piece : (i + 1) * piece]] for i in range(CHAINS)]
    for k in range(steps - 2):
        for i, chain in enumerate(chains):
            before_it = chains[i - 1]
            j = k if i > 0 else k - 1
            if j > 0:
                chain[k], before_it[j] = lax.optimization_barrier((chain[k], before_it[j]))
            chain.append(lax.ppermute(chain[k], PART, forth))
    last = lax.ppermute(jnp.concatenate([c[-1] for c in chains], axis=1), PART, forth)
    blocks = [[mine], [near]] + [[c[j] for c in chains] for j in range(1, steps - 1)] + [[last]]

    lens = jnp.concatenate([lengths, lengths_s])
    both = scored(blocks, (grads, grads_s), (inputs, inputs_s), lens, seat, routed, chips, total)
    mine_n = lengths.shape[0]
    fast = both[:mine_n] + swap(both[mine_n : 2 * mine_n])

    def general(fast, grads, inputs, live, raw):
        pair = counts.reshape(chips, 2)
        held = jnp.sum(pair, axis=1)
        chip_list = jnp.arange(chips, dtype=jnp.int32)
        before = jnp.cumsum(held) - held

        def step(k, carry):
            rows, out = carry
            source = jnp.remainder(z - k, chips)
            here = chip_list == source
            c0 = jnp.sum(jnp.where(here, pair[:, 0], 0))
            c1 = jnp.sum(jnp.where(here, pair[:, 1], 0))
            begin = jnp.sum(jnp.where(here, before, 0))
            valid = within < jnp.where(second, c1, c0)
            owner = (begin + within + jnp.where(second, c0, 0)) // RANK
            match = (owner[:, None] == jnp.arange(queries, dtype=jnp.int32)[None, :]) & valid[:, None]
            sums = sums_of(grads, inputs, live, rows[:, :ff], rows[:, ff:])
            out = out + exact(sums, match.astype(jnp.float32))
            return lax.ppermute(rows, "z", [(i, (i + 1) % chips) for i in range(chips)]), out

        return lax.fori_loop(0, chips, step, (raw, jnp.zeros_like(fast)))[1]

    return lax.cond(routed[1] == 1, lambda f, *_: f, general, fast, grads, inputs, live, raw)


def solution(mesh):
    groups, dp = mesh.devices.shape
    finer = Mesh(mesh.devices.reshape(groups, dp // 2, 2), SPLIT)
    return jax.shard_map(
        on_device,
        mesh=finer,
        in_specs=(
            P(SPLIT, None),
            P(SPLIT, None),
            P(SPLIT),
            P(SPLIT, None),
            P(SPLIT, None),
            P(SPLIT),
        ),
        out_specs=P(SPLIT, None),
        check_vma=False,
    )
```

```python
import jax
import jax.numpy as jnp
from jax import lax
from jax.experimental import pallas as pl
from jax.experimental.pallas import tpu as pltpu
from jax.sharding import Mesh
from jax.sharding import PartitionSpec as P

RANK = 32
LEN = 128
LANES = 128
ROWS_DEV = 4
REACH = 2
CHAINS = 2
PARTS = 3
STRIP = 2048
PART = ("z", "core")
SPLIT = ("groups", "z", "core")
CONTRACT = (((1,), (1,)), ((), ()))
FLAT = (((1,), (0,)), ((), ()))


def two_way(chips, hops):
    right = [(2 * i + 1, 2 * ((i + hops) % chips) + 1) for i in range(chips)]
    left = [(2 * i, 2 * ((i - hops) % chips)) for i in range(chips)]
    return right + left


def swap(x):
    return lax.ppermute(x, "core", [(0, 1), (1, 0)])


def dot(a, b):
    return lax.dot_general(a, b, CONTRACT, preferred_element_type=jnp.float32)


def sums_of(grads, inputs, live, left, right):
    joined = dot(grads, left) * dot(inputs, right) * live[:, None]
    return jnp.sum(joined.reshape(-1, LEN, joined.shape[1]), axis=1)


def exact(sums, assign):
    return jnp.dot(sums, assign, precision=lax.Precision.HIGHEST)


def log2(n):
    assert n & (n - 1) == 0
    return n.bit_length() - 1


def routed_rows(raw, one_hop, two_hops, counts, seat, block):
    chips = counts.shape[0] // 2
    slots, width = raw.shape
    cap = slots // 2
    strip = width // PARTS

    def body(counts_ref, seat_ref, raw_ref, one_ref, two_ref, out_ref, routed_ref, sel_ref, drift):
        @pl.when(pl.program_id(0) == 0)
        def _():
            z, first = seat_ref[0], seat_ref[1] == 0
            before, low, high = jnp.int32(0), jnp.int32(0), jnp.int32(0)
            for y in range(chips):
                drift[y] = before - block * y
                low = jnp.minimum(low, drift[y])
                before += counts_ref[2 * y] + counts_ref[2 * y + 1]
                high = jnp.maximum(high, before - 1 - block * y)
            shift = (block - 1 - low - high) >> 1
            routed_ref[0] = shift
            routed_ref[1] = (high - low <= block * (2 * REACH + 1) - 1).astype(jnp.int32)
            side = jnp.where(first, 1, -1)
            for h, size in enumerate((slots, 2 * block, block)):
                source = (z + side * h) & (chips - 1)
                c0, c1 = counts_ref[2 * source], counts_ref[2 * source + 1]
                start = drift[source] + shift + block * side * h
                slot = lax.broadcasted_iota(jnp.int32, (block, size), 1)
                place = lax.broadcasted_iota(jnp.int32, (block, size), 0)
                if h == 0:
                    second = slot >= cap
                    within = jnp.where(second, slot - cap, slot)
                    rank = within + jnp.where(second, c0, 0)
                    good = (within < jnp.where(second, c1, c0)) & (rank + jnp.where(first, 2 * slots, 0) < 2 * slots)
                else:
                    rank = slot + jnp.where(first, 0, c0 + c1 - size)
                    good = (rank >= 0) & (rank < c0 + c1)
                sel_ref[h, :, :size] = (good & (start + rank == place)).astype(jnp.float32)

        taken = None
        for h, ref in enumerate((raw_ref, one_ref, two_ref)):
            sel = sel_ref[h, :, : ref.shape[0]].astype(jnp.bfloat16)
            part = lax.dot_general(sel, ref[...], FLAT, preferred_element_type=jnp.float32)
            taken = part if taken is None else taken + part
        out_ref[...] = taken.astype(jnp.bfloat16)

    log2(chips)

    def spec(size):
        return pl.BlockSpec((size, strip), lambda k, *_: (0, k))

    return pl.pallas_call(
        body,
        out_shape=(jax.ShapeDtypeStruct((block, width), jnp.bfloat16), jax.ShapeDtypeStruct((2,), jnp.int32)),
        grid_spec=pltpu.PrefetchScalarGridSpec(
            num_scalar_prefetch=2,
            grid=(PARTS,),
            in_specs=[spec(slots), spec(2 * block), spec(block)],
            out_specs=(spec(block), pl.BlockSpec(memory_space=pltpu.SMEM)),
            scratch_shapes=[pltpu.VMEM((3, block, LANES), jnp.float32), pltpu.SMEM((chips,), jnp.int32)],
        ),
        compiler_params=pltpu.CompilerParams(dimension_semantics=("arbitrary",)),
    )(counts, seat, raw, one_hop, two_hops)


def scored(blocks, grads, inputs, lens, seat, routed, chips, total):
    block = blocks[0][0].shape[0]
    flat = [(s, p, len(pieces), x) for s, pieces in enumerate(blocks) for p, x in enumerate(pieces)]
    tokens, ff = grads[0].shape
    width = ff + inputs[0].shape[1]
    rows = len(blocks) * block
    queries = total // RANK
    sides = len(grads)
    examples = sides * tokens // LEN
    wide = ff // STRIP
    steps = width // STRIP

    def body(lens_ref, seat_ref, routed_ref, *refs):
        (g0, g1, i0, i1), refs = refs[:4], refs[4:]
        parts, refs = refs[: len(flat)], refs[len(flat) :]
        out_ref, held, left, right, sems = refs
        k = pl.program_id(0)

        def move(i):
            s, p, n, x = flat[i]
            target = held.at[pl.ds(s * block, block), pl.ds(p * (width // n), width // n)]
            return pltpu.make_async_copy(parts[i], target, sems.at[i])

        @pl.when(k == 0)
        def _():
            for i in range(len(flat)):
                move(i).start()
            left[...] = jnp.zeros_like(left)
            right[...] = jnp.zeros_like(right)

            for i, (_, p, _, _) in enumerate(flat):
                if p == 0:
                    move(i).wait()

        @pl.when(k == width // CHAINS // STRIP)
        def _():
            for i, (_, p, _, _) in enumerate(flat):
                if p > 0:
                    move(i).wait()

        strip = held[:, pl.ds(k * STRIP, STRIP)]

        @pl.when(k < wide)
        def _():
            left[:tokens, :] += dot(g0[...], strip)
            left[tokens:, :] += dot(g1[...], strip)

        @pl.when(k >= wide)
        def _():
            right[:tokens, :] += dot(i0[...], strip)
            right[tokens:, :] += dot(i1[...], strip)

        @pl.when(k == steps - 1)
        def _():
            token = lax.broadcasted_iota(jnp.int32, (LEN, rows), 0)
            sums = []
            for e in range(examples):
                at = pl.ds(e * LEN, LEN)
                joined = left[at, :] * right[at, :]
                sums.append(jnp.sum(jnp.where(token < lens_ref[e], joined, 0.0), axis=0, keepdims=True))
            sums = jnp.concatenate(sums + [jnp.zeros_like(sums[0])] * (8 - examples), axis=0)
            row = lax.broadcasted_iota(jnp.int32, (rows, queries), 0)
            hop = row >> log2(block)
            first = seat_ref[1] == 0
            chip = seat_ref[0] + jnp.where(first, hop, -hop)
            position = block * chip + (row & (block - 1)) - routed_ref[0]
            query = (position & (total - 1)) >> log2(RANK)
            counted = (hop >= jnp.where(first, 0, 1)) & (hop < jnp.where(first, chips // 2, chips))
            match = (query == lax.broadcasted_iota(jnp.int32, (rows, queries), 1)) & counted
            out_ref[...] = exact(sums, match.astype(jnp.float32))

    wide_spec = pl.BlockSpec((tokens, STRIP), lambda k, *_: (0, jnp.minimum(k, wide - 1)))
    slim_spec = pl.BlockSpec((tokens, STRIP), lambda k, *_: (0, jnp.maximum(k - wide, 0)))
    anywhere = pl.BlockSpec(memory_space=pl.ANY)
    return pl.pallas_call(
        body,
        out_shape=jax.ShapeDtypeStruct((8, queries), jnp.float32),
        grid_spec=pltpu.PrefetchScalarGridSpec(
            num_scalar_prefetch=3,
            grid=(steps,),
            in_specs=[wide_spec, wide_spec, slim_spec, slim_spec] + [anywhere] * len(flat),
            out_specs=pl.BlockSpec((8, queries), lambda k, *_: (0, 0)),
            scratch_shapes=[
                pltpu.VMEM((rows, width), jnp.bfloat16),
                pltpu.VMEM((sides * tokens, rows), jnp.float32),
                pltpu.VMEM((sides * tokens, rows), jnp.float32),
                pltpu.SemaphoreType.DMA((len(flat),)),
            ],
        ),
        compiler_params=pltpu.CompilerParams(dimension_semantics=("arbitrary",)),
    )(lens, seat, routed, *grads, *inputs, *[x for *_, x in flat])


def on_device(grads, inputs, lengths, left_rows, right_rows, owner_count):
    chips = lax.axis_size("z")
    z = lax.axis_index("z")
    core = lax.axis_index("core")
    devices = 2 * chips
    total = devices * ROWS_DEV
    queries = total // RANK
    block = total // chips
    cap = left_rows.shape[0]
    ff = left_rows.shape[1]
    width = ff + right_rows.shape[1]
    half = width // 2
    live = (jnp.arange(LEN, dtype=jnp.int32)[None, :] < lengths[:, None]).astype(jnp.float32).reshape(-1)

    own = jnp.concatenate([left_rows, right_rows], axis=1)
    packed = jnp.concatenate([own[:, :half], own[:, half:]], axis=0)
    small = jnp.concatenate([owner_count, lengths, jnp.zeros((LANES - 1 - lengths.shape[0],), jnp.int32)])
    notes = jnp.broadcast_to(small.astype(jnp.bfloat16)[None, :], (2 * cap, LANES))
    other = swap(jnp.concatenate([packed, notes], axis=1))
    notes = other[0, half:].astype(jnp.int32)
    other_count, lengths_s = notes[0], notes[1 : 1 + lengths.shape[0]]
    other = jnp.concatenate([other[:cap, :half], other[cap:, :half]], axis=1)
    first = core == 0
    raw = jnp.concatenate([jnp.where(first, own, other), jnp.where(first, other, own)], axis=0)

    n0 = jnp.where(first, owner_count[0], other_count)
    n1 = jnp.where(first, other_count, owner_count[0])
    slot = jnp.arange(2 * cap, dtype=jnp.int32)
    second = slot >= cap
    within = jnp.where(second, slot - cap, slot)
    valid = within < jnp.where(second, n1, n0)
    rank = jnp.where(valid, within + jnp.where(second, n0, 0), -1)
    lead = jnp.where(first, 0, n0 + n1 - 2 * block)
    edge_at = jnp.arange(2 * block, dtype=jnp.int32) + lead
    pick = (valid[None, :] & (rank[None, :] == edge_at[:, None])).astype(jnp.bfloat16)
    edge = lax.dot_general(pick, raw, FLAT, preferred_element_type=jnp.float32).astype(jnp.bfloat16)
    tip = jnp.where(first, edge[:block], edge[block:])
    device_list = jnp.arange(devices, dtype=jnp.int32)
    one_hop = lax.ppermute(edge, PART, two_way(chips, 1))
    two_hops = lax.ppermute(tip, PART, two_way(chips, 2))
    held_here = jnp.where(device_list == 2 * z, n0, jnp.where(device_list == 2 * z + 1, n1, 0))
    counts = lax.psum(held_here, "z")
    one_hop, two_hops, counts = lax.optimization_barrier((one_hop, two_hops, counts))
    seat = jnp.stack([z, core]).astype(jnp.int32)
    mine, routed = routed_rows(raw, one_hop, two_hops, counts, seat, block)
    mine = mine + swap(mine)
    mine, grads_t, inputs_t = lax.optimization_barrier((mine, grads, inputs))
    grads_s, inputs_s = swap(grads_t), swap(inputs_t)

    steps = chips // 2
    piece = width // CHAINS
    forth = two_way(chips, 1)
    near = lax.ppermute(mine, PART, forth)
    chains = [[near[:, i * piece : (i + 1) * piece]] for i in range(CHAINS)]
    for k in range(steps - 2):
        for i, chain in enumerate(chains):
            before_it = chains[i - 1]
            j = k if i > 0 else k - 1
            if j > 0:
                chain[k], before_it[j] = lax.optimization_barrier((chain[k], before_it[j]))
            chain.append(lax.ppermute(chain[k], PART, forth))
    last = lax.ppermute(jnp.concatenate([c[-1] for c in chains], axis=1), PART, forth)
    blocks = [[mine], [near]] + [[c[j] for c in chains] for j in range(1, steps - 1)] + [[last]]

    lens = jnp.concatenate([lengths, lengths_s])
    both = scored(blocks, (grads, grads_s), (inputs, inputs_s), lens, seat, routed, chips, total)
    mine_n = lengths.shape[0]
    fast = both[:mine_n] + swap(both[mine_n : 2 * mine_n])

    def general(fast, grads, inputs, live, raw):
        pair = counts.reshape(chips, 2)
        held = jnp.sum(pair, axis=1)
        chip_list = jnp.arange(chips, dtype=jnp.int32)
        before = jnp.cumsum(held) - held

        def step(k, carry):
            rows, out = carry
            source = jnp.remainder(z - k, chips)
            here = chip_list == source
            c0 = jnp.sum(jnp.where(here, pair[:, 0], 0))
            c1 = jnp.sum(jnp.where(here, pair[:, 1], 0))
            begin = jnp.sum(jnp.where(here, before, 0))
            valid = within < jnp.where(second, c1, c0)
            owner = (begin + within + jnp.where(second, c0, 0)) // RANK
            match = (owner[:, None] == jnp.arange(queries, dtype=jnp.int32)[None, :]) & valid[:, None]
            sums = sums_of(grads, inputs, live, rows[:, :ff], rows[:, ff:])
            out = out + exact(sums, match.astype(jnp.float32))
            return lax.ppermute(rows, "z", [(i, (i + 1) % chips) for i in range(chips)]), out

        return lax.fori_loop(0, chips, step, (raw, jnp.zeros_like(fast)))[1]

    return lax.cond(routed[1] == 1, lambda f, *_: f, general, fast, grads, inputs, live, raw)


def solution(mesh):
    groups, dp = mesh.devices.shape
    finer = Mesh(mesh.devices.reshape(groups, dp // 2, 2), SPLIT)
    return jax.shard_map(
        on_device,
        mesh=finer,
        in_specs=(
            P(SPLIT, None),
            P(SPLIT, None),
            P(SPLIT),
            P(SPLIT, None),
            P(SPLIT, None),
            P(SPLIT),
        ),
        out_specs=P(SPLIT, None),
        check_vma=False,
    )
```
